16 devices in a mesh: ey: 2 (over z), ex: 8 (over y, x, core).
Axes of the slice: x: 2, y: 2, z: 2, core: 2. Of those that a mesh axis runs over, the one named last changes fastest.
Arguments:
- x: bfloat16 [256, 2048], P(('ey', 'ex'))
- kv_k: bfloat16 [256, 256, 16, 128], P(('ey', 'ex'))
- kv_v: bfloat16 [256, 256, 16, 128], P(('ey', 'ex'))
- lens: int32 [256], P(('ey', 'ex'))
- topk_idx: int32 [256, 8], P(('ey', 'ex'))
- gates: float32 [256, 8], P(('ey', 'ex'))
- ln1: bfloat16 [2048], replicated
- ln2: bfloat16 [2048], replicated
- wq: bfloat16 [2048, 2048], replicated
- wo: bfloat16 [2048, 2048], replicated
- ws1: bfloat16 [2048, 1024], replicated
- ws3: bfloat16 [2048, 1024], replicated
- ws2: bfloat16 [1024, 2048], replicated
- w1: bfloat16 [64, 2048, 1024], P(('ey', 'ex'))
- w3: bfloat16 [64, 2048, 1024], P(('ey', 'ex'))
- w2: bfloat16 [64, 1024, 2048], P(('ey', 'ex'))
Outputs:
- output: bfloat16 [256, 2048], P(('ey', 'ex'))
All inputs are finite; a program needn't handle non-finite values.
Results may differ from the reference program's by a relative error of at most 0.0120205.
Values are sent between devices in bfloat16 or wider.
A program may use at most 1 GiB of HBM per device.

```python
import jax
import jax.numpy as jnp
from jax import lax

EY = 2
EX = 8
TOKENS = 16
LEN = 256
D = 2048
HEADS = 16
KV_HEADS = 16
HEAD = 128
FF = 1024
EXPERTS = 64
TOP = 8
ROWS_MAX = 2
CAP = 4
EPS = 1e-6
GATE_SCALE = 2.5

NDEV = EY * EX
NT = NDEV * TOKENS
EROW = EXPERTS // EY
NSLOT = EXPERTS * NDEV * CAP


def _normal(key, shape, scale):
    return (scale * jax.random.normal(key, shape, jnp.float32)).astype(jnp.bfloat16)


def _stack(key, n, shape, scale):
    return lax.map(lambda k: _normal(k, shape, scale), jax.random.split(key, n))


def _route(key):
    place_key, token_key = jax.random.split(key)
    places = jax.random.permutation(place_key, jnp.arange(EXPERTS, dtype=jnp.int32))
    half_count = EXPERTS // 2
    upper_span = EXPERTS - 1 - half_count
    offset = places - half_count
    square = offset * offset
    weight = jnp.where(offset < 0, 100 - (square * 78) // (half_count * half_count), 100 + (square * 350) // (upper_span * upper_span)).astype(jnp.uint32)
    row_of = jnp.arange(EXPERTS) // EROW

    def pick_one(one_key):
        order_key, count_key, noise_key = jax.random.split(one_key, 3)
        row_order = jax.random.permutation(order_key, EY)
        rows_used = jax.random.randint(count_key, (), 1, ROWS_MAX + 1)
        allowed = jnp.zeros((EY,), jnp.int32).at[row_order].set((jnp.arange(EY) < rows_used).astype(jnp.int32))
        noise_bits = jax.random.bits(noise_key, (EXPERTS,), jnp.uint32) >> 10
        waiting = jnp.where(allowed[row_of] > 0, noise_bits * weight, jnp.uint32(0xFFFFFFFF))
        return jnp.argsort(waiting)[:TOP]
    return jax.vmap(pick_one)(jax.random.split(token_key, NT)).astype(jnp.int32)


def setup_inputs(seed: int = 0) -> dict:
    ks = jax.random.split(jax.random.key(seed), 16)
    kd = jax.random.split(jax.random.fold_in(jax.random.key(seed), 7), 3)
    hd = HEADS * HEAD
    full = jax.random.uniform(kd[0], (NT,), jnp.float32) < 0.3
    short = jax.random.randint(kd[1], (NT,), 1, LEN // 8 + 1, jnp.int32)
    return {
        'x': _normal(ks[0], (NT, D), 1.0),
        'kv_k': _stack(ks[1], NT, (LEN, KV_HEADS, HEAD), 2.0),
        'kv_v': _stack(ks[2], NT, (LEN, KV_HEADS, HEAD), 1.0),
        'lens': jnp.where(full, LEN, short).astype(jnp.int32),
        'topk_idx': _route(kd[2]),
        'gates': GATE_SCALE * jax.nn.softmax(0.5 * jax.random.normal(ks[5], (NT, TOP), jnp.float32), axis=-1),
        'ln1': (1.0 + 0.1 * jax.random.normal(ks[6], (D,), jnp.float32)).astype(jnp.bfloat16),
        'ln2': (1.0 + 0.1 * jax.random.normal(ks[7], (D,), jnp.float32)).astype(jnp.bfloat16),
        'wq': _normal(ks[8], (D, hd), D ** -0.5),
        'wo': _normal(ks[9], (hd, D), hd ** -0.5),
        'ws1': _normal(ks[10], (D, FF), D ** -0.5),
        'ws3': _normal(ks[11], (D, FF), D ** -0.5),
        'ws2': _normal(ks[12], (FF, D), FF ** -0.5),
        'w1': _stack(ks[13], EXPERTS, (D, FF), D ** -0.5),
        'w3': _stack(ks[14], EXPERTS, (D, FF), D ** -0.5),
        'w2': _stack(ks[15], EXPERTS, (FF, D), FF ** -0.5),
    }


def _rms(v, w):
    v = v.astype(jnp.float32)
    r = lax.rsqrt(jnp.mean(v * v, axis=-1, keepdims=True) + EPS)
    return (v * r * w.astype(jnp.float32)).astype(jnp.bfloat16)


def _ffn(u, w1, w3, w2):
    g = jnp.dot(u, w1, preferred_element_type=jnp.float32)
    v = jnp.dot(u, w3, preferred_element_type=jnp.float32)
    z = (jax.nn.silu(g) * v).astype(jnp.bfloat16)
    return jnp.dot(z, w2, preferred_element_type=jnp.float32).astype(jnp.bfloat16)


def _attn(x, kk, vv, lens, ln1, wq, wo):
    b = x.shape[0]
    a = _rms(x, ln1)
    q = jnp.dot(a, wq, preferred_element_type=jnp.float32).astype(jnp.bfloat16)
    q = q.reshape(b, KV_HEADS, HEADS // KV_HEADS, HEAD).astype(jnp.float32)
    s = jnp.einsum('bkgd,blkd->bkgl', q, kk.astype(jnp.float32)) * HEAD ** -0.5
    valid = jnp.arange(LEN)[None, :] < lens[:, None]
    s = jnp.where(valid[:, None, None, :], s, -jnp.inf)
    p = jax.nn.softmax(s, axis=-1).astype(jnp.bfloat16).astype(jnp.float32)
    o = jnp.einsum('bkgl,blkd->bkgd', p, vv.astype(jnp.float32)).astype(jnp.bfloat16)
    attn = jnp.dot(o.reshape(b, HEADS * HEAD), wo, preferred_element_type=jnp.float32)
    return (x.astype(jnp.float32) + attn).astype(jnp.bfloat16)


def _slots(topk_idx, gates):
    chosen = (topk_idx[:, :, None] == jnp.arange(EXPERTS)[None, None, :]).any(axis=1).astype(jnp.int32)
    chosen = chosen.reshape(NDEV, TOKENS, EXPERTS)
    before = (jnp.cumsum(chosen, axis=1) - chosen).reshape(NT, EXPERTS)
    rank = jnp.take_along_axis(before, topk_idx, axis=1)
    src = (jnp.arange(NT, dtype=jnp.int32) // TOKENS)[:, None]
    pos = jnp.where(rank < CAP, (topk_idx * NDEV + src) * CAP + rank, NSLOT).reshape(-1)
    tok = jnp.broadcast_to(jnp.arange(NT, dtype=jnp.int32)[:, None], (NT, TOP)).reshape(-1)
    slot_tok = jnp.full((NSLOT,), NT, jnp.int32).at[pos].set(tok, mode='drop')
    slot_gate = jnp.zeros((NSLOT,), jnp.float32).at[pos].set(gates.reshape(-1), mode='drop')
    return slot_tok.reshape(EXPERTS, NDEV * CAP), slot_gate.reshape(EXPERTS, NDEV * CAP)


def reference(x, kv_k, kv_v, lens, topk_idx, gates, ln1, ln2, wq, wo, ws1, ws3, ws2, w1, w3, w2):
    per_dev = lambda a: a.reshape((NDEV, TOKENS) + a.shape[1:])
    h = lax.map(lambda t: _attn(t[0], t[1], t[2], t[3], ln1, wq, wo),
                (per_dev(x), per_dev(kv_k), per_dev(kv_v), per_dev(lens))).reshape(NT, D)
    u = _rms(h, ln2)
    slot_tok, slot_gate = _slots(topk_idx, gates)
    u_pad = jnp.concatenate([u, jnp.zeros((1, D), jnp.bfloat16)], axis=0)

    def expert(acc, xs):
        tok, gate, a1, a3, a2 = xs
        e = _ffn(u_pad[tok], a1, a3, a2)
        return acc.at[tok].add(gate[:, None] * e.astype(jnp.float32)), None

    routed, _ = lax.scan(expert, jnp.zeros((NT + 1, D), jnp.float32), (slot_tok, slot_gate, w1, w3, w2))
    y = h.astype(jnp.float32) + _ffn(u, ws1, ws3, ws2).astype(jnp.float32) + routed[:NT]
    return y.astype(jnp.bfloat16)
```

```python
import functools

import jax
import jax.numpy as jnp
from jax import lax
from jax.experimental import pallas as pl
from jax.experimental.pallas import tpu as pltpu
from jax.sharding import PartitionSpec as P

EPS = 1e-6
BF = jnp.bfloat16
F32 = jnp.float32
I32 = jnp.int32
MESH = pl.DeviceIdType.MESH
VMEM_LIMIT = 60 * 1024 * 1024

SHORT = 32


def _iota(shape, dim):
    return lax.broadcasted_iota(I32, shape, dim)


def _dot(a, b):
    return jnp.dot(a, b, preferred_element_type=F32)


def _rms(v, w):
    v = v.astype(F32)
    r = lax.rsqrt(jnp.mean(v * v, axis=-1, keepdims=True) + EPS)
    return (v * r * w.astype(F32)).astype(BF)


def _attn_kernel(lens, x, ln1, ln2, kk, vv, wq, wo, h_out, u_out,
                 kbuf, vbuf, wqb, wob, q3, o3, posd, longs,
                 wsem, ssem, lsem):
    b, heads, dh = q3.shape
    rows = kbuf.shape[1]
    short = SHORT * heads
    d = x.shape[1]
    nw = wsem.shape[1]
    cw = d // nw
    scale = dh ** -0.5

    def wcopy(i, n):
        src, dst = ((wq, wqb), (wo, wob))[i]
        return pltpu.make_async_copy(src.at[:, pl.ds(n * cw, cw)], dst.at[:, pl.ds(n * cw, cw)], wsem.at[i, n])

    def scopy(i, t):
        src, dst = ((kk, kbuf), (vv, vbuf))[i]
        return pltpu.make_async_copy(src.at[t, pl.ds(0, short)], dst.at[t, pl.ds(0, short)], ssem.at[i])

    def lcopy(i, t):
        src, dst = ((kk, kbuf), (vv, vbuf))[i]
        rest = pl.ds(short, rows - short)
        return pltpu.make_async_copy(src.at[t, rest], dst.at[t, rest], lsem.at[i, t])

    for n in range(nw):
        wcopy(0, n).start()
    for t in range(b):
        scopy(0, t).start()
        scopy(1, t).start()

    def scan(t, n):
        @pl.when(lens[t] > SHORT)
        def _():
            longs[n] = t
            lcopy(0, t).start()
            lcopy(1, t).start()
        return n + (lens[t] > SHORT).astype(I32)

    nlong = lax.fori_loop(0, b, scan, jnp.int32(0))
    for n in range(nw):
        wcopy(1, n).start()

    col = _iota((heads, rows), 1)
    posd[...] = jnp.where(col % heads == _iota((heads, rows), 0), col // heads, jnp.int32(1 << 20))

    a = _rms(x[...], ln1[...])
    for n in range(nw):
        wcopy(0, n).wait()
        q = _dot(a, wqb[:, n * cw:(n + 1) * cw]).astype(BF).astype(F32)
        for i in range(cw // dh):
            q3[:, n * (cw // dh) + i, :] = q[:, i * dh:(i + 1) * dh]

    def scores(t, m):
        qt = q3[t].astype(BF)
        s = lax.dot_general(qt, kbuf[t, :m], (((1,), (1,)), ((), ())), preferred_element_type=F32)
        s = jnp.where(posd[:, :m] < lens[t], s * scale, -jnp.inf)
        top = jnp.max(s, axis=-1, keepdims=True)
        e = jnp.exp(s - top)
        return (e / jnp.sum(e, axis=-1, keepdims=True)).astype(BF)

    def attend(ts, m):
        ps = [scores(t, m) for t in ts]
        for t, p in zip(ts, ps):
            o3[t] = _dot(p, vbuf[t, :m]).astype(BF).astype(F32)

    for t in range(b):
        scopy(0, t).wait()
        scopy(1, t).wait()
    group = 8
    for t0 in range(0, b, group):
        attend(list(range(t0, t0 + group)), short)

    def long_pair(j, carry):
        first = 2 * j
        second = jnp.minimum(first + 1, nlong - 1)
        t0, t1 = longs[first], longs[second]
        lcopy(0, t0).wait()
        lcopy(1, t0).wait()

        @pl.when(second > first)
        def _():
            lcopy(0, t1).wait()
            lcopy(1, t1).wait()
        attend([t0, t1], rows)
        return carry

    lax.fori_loop(0, (nlong + 1) // 2, long_pair, 0)

    o = jnp.concatenate([o3[:, i, :].astype(BF) for i in range(heads)], axis=1)
    for n in range(nw):
        wcopy(1, n).wait()
        sl = slice(n * cw, (n + 1) * cw)
        h_out[:, sl] = (x[:, sl].astype(F32) + _dot(o, wob[:, sl])).astype(BF)
    u_out[...] = _rms(h_out[...], ln2[...])


def _attention(x, kk, vv, lens, ln1, ln2, wq, wo):
    b, d = x.shape
    _, l, heads, dh = kk.shape
    rows = l * heads
    vm = pl.BlockSpec(memory_space=pltpu.VMEM)
    hbm = pl.BlockSpec(memory_space=pl.ANY)
    nbytes = 2 * (2 * b * rows * dh + 2 * d * d)
    return pl.pallas_call(
        _attn_kernel,
        out_shape=[jax.ShapeDtypeStruct((b, d), BF)] * 2,
        in_specs=[pl.BlockSpec(memory_space=pltpu.SMEM), vm, vm, vm, hbm, hbm, hbm, hbm],
        out_specs=[vm, vm],
        scratch_shapes=[
            pltpu.VMEM((b, rows, dh), BF),
            pltpu.VMEM((b, rows, dh), BF),
            pltpu.VMEM((d, d), BF),
            pltpu.VMEM((d, d), BF),
            pltpu.VMEM((b, heads, dh), F32),
            pltpu.VMEM((b, heads, dh), F32),
            pltpu.VMEM((heads, rows), I32),
            pltpu.SMEM((b,), I32),
            pltpu.SemaphoreType.DMA((2, 4)),
            pltpu.SemaphoreType.DMA((2,)),
            pltpu.SemaphoreType.DMA((2, b)),
        ],
        compiler_params=pltpu.CompilerParams(vmem_limit_bytes=VMEM_LIMIT),
        cost_estimate=pl.CostEstimate(flops=4 * b * d * d, bytes_accessed=nbytes, transcendentals=0),
        name='attention',
    )(lens, x, ln1.reshape(1, d), ln2.reshape(1, d),
      kk.reshape(b, rows, dh), vv.reshape(b, rows, dh), wq, wo)


def _moe_kernel(cap, h, u, topk_t, topk, gates, ws1, ws3, ws2, w1, w3, w2, y,
                wab, wcb, place, praw, perm, ug, xin, oscr, ret, gmat,
                asem, csem, psend, precv, usend, urecv, vsend, vrecv,
                rsend, rrecv, tsend, trecv):
    b, d = h.shape
    k = topk.shape[1]
    edev = w1.shape[0]
    ff = w1.shape[2]
    ndev = praw.shape[0]
    nchip = ndev // 2
    ntok = ndev * b
    slots = edev * cap
    nslot = ndev * slots
    erow = ndev * cap
    ey, ex = lax.axis_index('ey'), lax.axis_index('ex')
    nex = nchip
    iy = lax.div(ex, 4)
    ix = lax.div(ex, 2) - 2 * iy
    core = lax.rem(ex, 2)
    me = ey * nex + ex
    chip_me = lax.div(me, 2)

    flip = lambda i, by: 1 - i if by else i
    peers = {}
    for dist in range(nchip):
        pz, py, px = flip(ey, dist // 4), flip(iy, dist // 2 % 2), flip(ix, dist % 2)
        for oc in range(2):
            pex = py * 4 + px * 2 + flip(core, oc)
            peers[dist, oc] = ((pz, pex), pz * nex + pex)
    chips = [lax.div(peers[dist, 0][1], 2) for dist in range(nchip)]

    def peer(dist, other_core):
        return peers[dist, other_core]

    def acopy(e, i):
        return pltpu.make_async_copy((w1, w3)[i].at[e], wab.at[2 * e + i], asem.at[e, i])

    def ccopy(e):
        return pltpu.make_async_copy(w2.at[e], wcb.at[e], csem.at[e])

    def shared_copies():
        return [pltpu.make_async_copy(ws1, wab.at[0], asem.at[edev, 0]),
                pltpu.make_async_copy(ws3, wab.at[1], asem.at[edev, 1]),
                pltpu.make_async_copy(ws2, wcb.at[0], csem.at[edev])]

    for e in range(edev):
        acopy(e, 0).start()
        acopy(e, 1).start()
        ccopy(e).start()

    barrier = pltpu.get_barrier_semaphore()
    for dist in range(nchip):
        for oc in range(2):
            if dist or oc:
                pl.semaphore_signal(barrier, inc=1, device_id=peer(dist, oc)[0], device_id_type=MESH)

    row, colm = _iota((nslot, ntok), 0), _iota((nslot, ntok), 1)
    row_e = lax.div(row, cap)
    row_r = (row - row_e * cap).astype(F32)
    hit = jnp.zeros((nslot, ntok), F32)
    for j in range(k):
        hit = jnp.where(row_e == topk_t[j:j + 1, :], 1.0, hit)
    ra, ca = _iota((ntok, ntok), 0), _iota((ntok, ntok), 1)
    cb = lax.div(ca, b)
    earlier = jnp.where((lax.div(ra, b) == cb) & (ra < ca), 1.0, 0.0).astype(BF)
    before = _dot(hit.astype(BF), earlier)
    mine = jnp.where((before == row_r) & (lax.div(colm, b) == me), hit, 0.0)
    place[...] = mine.astype(BF).reshape(ndev, slots, ntok)

    nret = ndev * edev * 2 * cap
    lane = _iota((b, nret), 1)
    glob = lax.div(lane, 2 * cap)
    half = lax.div(lane, cap)
    lane_r = (lane - half * cap).astype(F32)
    got = jnp.zeros((b, nret), F32)
    gate = jnp.zeros((b, nret), F32)
    for j in range(k):
        same = glob == topk[:, j:j + 1]
        got = jnp.where(same, 1.0, got)
        gate = jnp.where(same, gates[:, j:j + 1], gate)
    lower = jnp.where(_iota((b, b), 1) < _iota((b, b), 0), 1.0, 0.0).astype(BF)
    prior = _dot(lower, got.astype(BF))
    keep = (prior == lane_r) & (half - 2 * glob == core)
    gate = jnp.where(keep, gate, 0.0)
    g1 = gate.astype(BF)
    rest = gate - g1.astype(F32)
    g2 = rest.astype(BF)
    g3 = (rest - g2.astype(F32)).astype(BF)
    gmat[0:b] = g1
    gmat[b:2 * b] = g2
    gmat[2 * b:3 * b] = g3

    ug[me] = u[...]
    praw[me] = place[me]

    pl.semaphore_wait(barrier, ndev - 1)

    def ucopy(dist):
        return pltpu.make_async_remote_copy(
            src_ref=u, dst_ref=ug.at[me], send_sem=usend.at[dist], recv_sem=urecv.at[dist],
            device_id=peer(dist, 0)[0], device_id_type=MESH)

    def vcopy(dist):
        src = peer(dist, 0)[1]
        return pltpu.make_async_remote_copy(
            src_ref=u if dist == 0 else ug.at[src], dst_ref=ug.at[src],
            send_sem=vsend.at[dist], recv_sem=vrecv.at[dist],
            device_id=peer(0, 1)[0], device_id_type=MESH)

    def pcopy(dist, oc):
        to, idx = peer(dist, oc)
        return pltpu.make_async_remote_copy(
            src_ref=place.at[idx], dst_ref=praw.at[me],
            send_sem=psend.at[2 * dist + oc], recv_sem=precv.at[2 * dist + oc],
            device_id=to, device_id_type=MESH)

    others = [(dist, oc) for dist in range(nchip) for oc in range(2) if dist or oc]
    order = [7, 6, 5, 3, 4, 2, 1]
    for dist in order:
        ucopy(dist).start()
    vcopy(0).start()
    for dist, oc in others:
        pcopy(dist, oc).start()
    for dist, oc in others:
        pcopy(dist, oc).wait_recv()

    rp, cp = _iota((nslot, nslot), 0), _iota((nslot, nslot), 1)
    rsrc, rexp = lax.div(rp, cap), lax.div(rp, erow)
    want = (rsrc - rexp * ndev) * slots + rexp * cap + (rp - rsrc * cap)
    perm[...] = _dot(jnp.where(want == cp, 1.0, 0.0).astype(BF), praw[...].reshape(nslot, ntok)).astype(BF)

    for dist in [4, 2, 1, 6, 5, 3, 7]:
        ucopy(dist).wait_recv()
        vcopy(dist).start()
    for dist in range(nchip):
        vcopy(dist).wait_recv()

    nx = 4
    cx = d // nx
    for n in range(nx):
        sl = slice(n * cx, (n + 1) * cx)
        xin[:, :, sl] = _dot(perm[...], ug[:, :, sl].reshape(ntok, cx)).astype(BF).reshape(edev, erow, cx)

    def rcopy(e, dist):
        chip = chips[dist]
        return pltpu.make_async_remote_copy(
            src_ref=oscr.at[e, chip], dst_ref=ret.at[me * edev + e],
            send_sem=rsend.at[e, dist], recv_sem=rrecv.at[e, dist],
            device_id=peer(dist, 0)[0], device_id_type=MESH)

    def tcopy(e, dist):
        src = peer(dist, 0)[1]
        at = src * edev + e
        return pltpu.make_async_remote_copy(
            src_ref=oscr.at[e, chip_me] if dist == 0 else ret.at[at], dst_ref=ret.at[at],
            send_sem=tsend.at[e, dist], recv_sem=trecv.at[e, dist],
            device_id=peer(0, 1)[0], device_id_type=MESH)

    def ffn(uv, i1, i3, i2, store):
        nz = 2
        cz = ff // nz
        zs = []
        for n in range(nz):
            sl = slice(n * cz, (n + 1) * cz)
            g = _dot(uv, wab[i1, :, sl])
            v = _dot(uv, wab[i3, :, sl])
            zs.append((g / (1.0 + jnp.exp(-g)) * v).astype(BF))
        z = jnp.concatenate(zs, axis=1)
        ny = 4
        cy = d // ny
        return z, ny, cy

    def forward(e):
        for dist in [4, 2, 1, 6, 5, 3, 7]:
            rcopy(e, dist).wait_recv()
            tcopy(e, dist).start()

    for e in range(edev):
        acopy(e, 0).wait()
        acopy(e, 1).wait()
        z, ny, cy = ffn(xin[e], 2 * e, 2 * e + 1, e, None)
        ccopy(e).wait()
        for n in range(ny):
            sl = slice(n * cy, (n + 1) * cy)
            oscr[e, :, :, sl] = _dot(z, wcb[e, :, sl]).astype(BF).reshape(nchip, 2 * cap, cy)
        if e == 0:
            for c in shared_copies():
                c.start()
        for dist in order:
            rcopy(e, dist).start()
        tcopy(e, 0).start()
        ret[me * edev + e] = oscr[e, chip_me]
        if e > 0:
            forward(e - 1)

    sa, sb, sc = shared_copies()
    sa.wait()
    sb.wait()
    z, ny, cy = ffn(u[...], 0, 1, 0, None)
    sc.wait()
    shared = [_dot(z, wcb[0, :, n * cy:(n + 1) * cy]).astype(BF) for n in range(ny)]

    forward(edev - 1)
    for e in range(edev):
        for dist in range(nchip):
            tcopy(e, dist).wait_recv()
    for n in range(ny):
        sl = slice(n * cy, (n + 1) * cy)
        r = _dot(gmat[...], ret[:, :, sl].reshape(nret, cy))
        routed = r[0:b] + r[b:2 * b] + r[2 * b:3 * b]
        y[:, sl] = (h[:, sl].astype(F32) + shared[n].astype(F32) + routed).astype(BF)

    for dist, oc in others:
        pcopy(dist, oc).wait_send()
    for dist in range(1, nchip):
        ucopy(dist).wait_send()
    for dist in range(nchip):
        vcopy(dist).wait_send()
    for e in range(edev):
        for dist in range(1, nchip):
            rcopy(e, dist).wait_send()
        for dist in range(nchip):
            tcopy(e, dist).wait_send()


def _moe(h, u, topk, gates, ws1, ws3, ws2, w1, w3, w2, ndev, cap):
    b, d = h.shape
    edev, _, ff = w1.shape
    nchip = ndev // 2
    slots = edev * cap
    vm = pl.BlockSpec(memory_space=pltpu.VMEM)
    hbm = pl.BlockSpec(memory_space=pl.ANY)
    dma = pltpu.SemaphoreType.DMA
    topk_t = jnp.tile(topk.T, (1, ndev))
    return pl.pallas_call(
        functools.partial(_moe_kernel, cap),
        out_shape=jax.ShapeDtypeStruct((b, d), BF),
        in_specs=[vm] * 5 + [hbm] * 6,
        out_specs=vm,
        scratch_shapes=[
            pltpu.VMEM((2 * edev, d, ff), BF),
            pltpu.VMEM((edev, ff, d), BF),
            pltpu.VMEM((ndev, slots, ndev * b), BF),
            pltpu.VMEM((ndev, slots, ndev * b), BF),
            pltpu.VMEM((ndev * slots, ndev * b), BF),
            pltpu.VMEM((ndev, b, d), BF),
            pltpu.VMEM((edev, ndev * cap, d), BF),
            pltpu.VMEM((edev, nchip, 2 * cap, d), BF),
            pltpu.VMEM((ndev * edev, 2 * cap, d), BF),
            pltpu.VMEM((3 * b, ndev * edev * 2 * cap), BF),
            dma((edev + 1, 2)), dma((edev + 1,)),
            dma((ndev,)), dma((ndev,)),
            dma((nchip,)), dma((nchip,)), dma((nchip,)), dma((nchip,)),
            dma((edev, nchip)), dma((edev, nchip)), dma((edev, nchip)), dma((edev, nchip)),
        ],
        compiler_params=pltpu.CompilerParams(
            collective_id=0, has_side_effects=True, vmem_limit_bytes=VMEM_LIMIT),
        cost_estimate=pl.CostEstimate(
            flops=6 * (edev * ndev * cap + b) * d * ff, bytes_accessed=6 * (edev + 1) * d * ff, transcendentals=0),
        name='experts',
    )(h, u, topk_t, topk, gates, ws1, ws3, ws2, w1, w3, w2)


def solution(mesh):
    ndev = mesh.shape['ey'] * mesh.shape['ex']
    rows = P(('ey', 'ex'))
    rep = P()

    def local(x, kv_k, kv_v, lens, topk_idx, gates, ln1, ln2, wq, wo, ws1, ws3, ws2, w1, w3, w2):
        cap = 4
        h, u = _attention(x, kv_k, kv_v, lens, ln1, ln2, wq, wo)
        return _moe(h, u, topk_idx, gates, ws1, ws3, ws2, w1, w3, w2, ndev, cap)

    return jax.shard_map(
        local, mesh=mesh,
        in_specs=(rows, rows, rows, rows, rows, rows, rep, rep, rep, rep, rep, rep, rep, rows, rows, rows),
        out_specs=rows, check_vma=False)
```

```python
import functools

import jax
import jax.numpy as jnp
from jax import lax
from jax.experimental import pallas as pl
from jax.experimental.pallas import tpu as pltpu
from jax.sharding import PartitionSpec as P

EPS = 1e-6
BF = jnp.bfloat16
F32 = jnp.float32
I32 = jnp.int32
MESH = pl.DeviceIdType.MESH
VMEM_LIMIT = 60 * 1024 * 1024

SHORT = 32


def _iota(shape, dim):
    return lax.broadcasted_iota(I32, shape, dim)


def _dot(a, b):
    return jnp.dot(a, b, preferred_element_type=F32)


def _rms(v, w):
    v = v.astype(F32)
    r = lax.rsqrt(jnp.mean(v * v, axis=-1, keepdims=True) + EPS)
    w = w.astype(F32)
    n = w.shape[1]
    parts = [(v[:, i * n:(i + 1) * n] * r * w[i:i + 1, :]).astype(BF) for i in range(w.shape[0])]
    return jnp.concatenate(parts, axis=1)


def _attn_kernel(lens, x, ln1, ln2, kk, vv, wq, wo, h_out, u_out,
                 kbuf, vbuf, wqb, wob, q3, o3, posd, longs,
                 wsem, ssem, lsem):
    b, heads, dh = q3.shape
    rows = kbuf.shape[1]
    short = SHORT * heads
    d = x.shape[1]
    nw = wsem.shape[1]
    cw = d // nw
    scale = dh ** -0.5

    def wcopy(i, n):
        src, dst = ((wq, wqb), (wo, wob))[i]
        return pltpu.make_async_copy(src.at[:, pl.ds(n * cw, cw)], dst.at[:, pl.ds(n * cw, cw)], wsem.at[i, n])

    def scopy(i, t):
        src, dst = ((kk, kbuf), (vv, vbuf))[i]
        return pltpu.make_async_copy(src.at[t, pl.ds(0, short)], dst.at[t, pl.ds(0, short)], ssem.at[i])

    def lcopy(i, t):
        src, dst = ((kk, kbuf), (vv, vbuf))[i]
        rest = pl.ds(short, rows - short)
        return pltpu.make_async_copy(src.at[t, rest], dst.at[t, rest], lsem.at[i, t])

    for n in range(nw):
        wcopy(0, n).start()
    for t in range(b):
        scopy(0, t).start()
        scopy(1, t).start()

    def scan(t, n):
        @pl.when(lens[t] > SHORT)
        def _():
            longs[n] = t
            lcopy(0, t).start()
            lcopy(1, t).start()
        return n + (lens[t] > SHORT).astype(I32)

    nlong = lax.fori_loop(0, b, scan, jnp.int32(0))
    for n in range(nw):
        wcopy(1, n).start()

    col = _iota((heads, rows), 1)
    posd[...] = jnp.where(col % heads == _iota((heads, rows), 0), col // heads, jnp.int32(1 << 20))

    a = _rms(x[...], ln1[...])
    for n in range(nw):
        wcopy(0, n).wait()
        q = _dot(a, wqb[:, n * cw:(n + 1) * cw]).astype(BF).astype(F32)
        for i in range(cw // dh):
            q3[:, n * (cw // dh) + i, :] = q[:, i * dh:(i + 1) * dh]

    def scores(t, m):
        qt = q3[t].astype(BF)
        s = lax.dot_general(qt, kbuf[t, :m], (((1,), (1,)), ((), ())), preferred_element_type=F32)
        s = jnp.where(posd[:, :m] < lens[t], s * scale, -jnp.inf)
        top = jnp.max(s, axis=-1, keepdims=True)
        e = jnp.exp(s - top)
        return (e / jnp.sum(e, axis=-1, keepdims=True)).astype(BF)

    def attend(ts, m):
        ps = [scores(t, m) for t in ts]
        for t, p in zip(ts, ps):
            o3[t] = _dot(p, vbuf[t, :m]).astype(BF).astype(F32)

    for t in range(b):
        scopy(0, t).wait()
        scopy(1, t).wait()
    group = 8
    for t0 in range(0, b, group):
        attend(list(range(t0, t0 + group)), short)

    def long_pair(j, carry):
        first = 2 * j
        second = jnp.minimum(first + 1, nlong - 1)
        t0, t1 = longs[first], longs[second]
        lcopy(0, t0).wait()
        lcopy(1, t0).wait()

        @pl.when(second > first)
        def _():
            lcopy(0, t1).wait()
            lcopy(1, t1).wait()
        attend([t0, t1], rows)
        return carry

    lax.fori_loop(0, (nlong + 1) // 2, long_pair, 0)

    o = jnp.concatenate([o3[:, i, :].astype(BF) for i in range(heads)], axis=1)
    for n in range(nw):
        wcopy(1, n).wait()
        sl = slice(n * cw, (n + 1) * cw)
        h_out[:, sl] = (x[:, sl].astype(F32) + _dot(o, wob[:, sl])).astype(BF)
    u_out[...] = _rms(h_out[...], ln2[...])


def _attention(x, kk, vv, lens, ln1, ln2, wq, wo):
    b, d = x.shape
    _, l, heads, dh = kk.shape
    rows = l * heads
    vm = pl.BlockSpec(memory_space=pltpu.VMEM)
    hbm = pl.BlockSpec(memory_space=pl.ANY)
    nbytes = 2 * (2 * b * rows * dh + 2 * d * d)
    return pl.pallas_call(
        _attn_kernel,
        out_shape=[jax.ShapeDtypeStruct((b, d), BF)] * 2,
        in_specs=[pl.BlockSpec(memory_space=pltpu.SMEM), vm, vm, vm, hbm, hbm, hbm, hbm],
        out_specs=[vm, vm],
        scratch_shapes=[
            pltpu.VMEM((b, rows, dh), BF),
            pltpu.VMEM((b, rows, dh), BF),
            pltpu.VMEM((d, d), BF),
            pltpu.VMEM((d, d), BF),
            pltpu.VMEM((b, heads, dh), F32),
            pltpu.VMEM((b, heads, dh), F32),
            pltpu.VMEM((heads, rows), I32),
            pltpu.SMEM((b,), I32),
            pltpu.SemaphoreType.DMA((2, 4)),
            pltpu.SemaphoreType.DMA((2,)),
            pltpu.SemaphoreType.DMA((2, b)),
        ],
        compiler_params=pltpu.CompilerParams(vmem_limit_bytes=VMEM_LIMIT),
        cost_estimate=pl.CostEstimate(flops=4 * b * d * d, bytes_accessed=nbytes, transcendentals=0),
        name='attention',
    )(lens, x, ln1.reshape(d // 128, 128), ln2.reshape(d // 128, 128),
      kk.reshape(b, rows, dh), vv.reshape(b, rows, dh), wq, wo)


def _moe_kernel(cap, h, u, topk_t, gates_t, ws1, ws3, ws2, w1, w3, w2, y,
                wab, wcb, tmine, tall, perm, ug, xin, oscr, ret, gmat,
                asem, csem, psend, precv, qsend, qrecv, usend, urecv, vsend, vrecv,
                rsend, rrecv, tsend, trecv):
    b, d = h.shape
    k = topk_t.shape[0]
    edev = w1.shape[0]
    ff = w1.shape[2]
    ndev = ug.shape[0]
    nchip = ndev // 2
    ntok = ndev * b
    slots = edev * cap
    nslot = ndev * slots
    erow = ndev * cap
    ey, ex = lax.axis_index('ey'), lax.axis_index('ex')
    nex = nchip
    iy = lax.div(ex, 4)
    ix = lax.div(ex, 2) - 2 * iy
    core = lax.rem(ex, 2)
    me = ey * nex + ex
    chip_me = lax.div(me, 2)

    flip = lambda i, by: 1 - i if by else i
    peers = {}
    for dist in range(nchip):
        pz, py, px = flip(ey, dist // 4), flip(iy, dist // 2 % 2), flip(ix, dist % 2)
        for oc in range(2):
            pex = py * 4 + px * 2 + flip(core, oc)
            peers[dist, oc] = ((pz, pex), pz * nex + pex)
    chips = [lax.div(peers[dist, 0][1], 2) for dist in range(nchip)]

    def peer(dist, other_core):
        return peers[dist, other_core]

    def acopy(e, i):
        return pltpu.make_async_copy((w1, w3)[i].at[e], wab.at[2 * e + i], asem.at[e, i])

    def ccopy(e):
        return pltpu.make_async_copy(w2.at[e], wcb.at[e], csem.at[e])

    def shared_copies():
        return [pltpu.make_async_copy(ws1, wab.at[0], asem.at[edev, 0]),
                pltpu.make_async_copy(ws3, wab.at[1], asem.at[edev, 1]),
                pltpu.make_async_copy(ws2, wcb.at[0], csem.at[edev])]

    for e in range(edev):
        acopy(e, 0).start()
        acopy(e, 1).start()
        ccopy(e).start()

    barrier = pltpu.get_barrier_semaphore()
    for dist in range(nchip):
        for oc in range(2):
            if dist or oc:
                pl.semaphore_signal(barrier, inc=1, device_id=peer(dist, oc)[0], device_id_type=MESH)

    lanes = tmine.shape[1]
    tk = topk_t[...].astype(F32)
    rep_r, rep_c = _iota((b, lanes), 0), _iota((b, lanes), 1)
    block = me - lax.div(me, lanes // b) * (lanes // b)
    spread = jnp.where(rep_c - block * b == rep_r, 1.0, 0.0).astype(BF)
    tmine[...] = _dot(tk.astype(BF), spread)
    tall[me] = tmine[...]
    ug[me] = u[...]

    nret = ndev * edev * 2 * cap
    lane = _iota((b, nret), 1)
    glob = lax.div(lane, 2 * cap)
    half = lax.div(lane, cap)
    lane_r = (lane - half * cap).astype(F32)
    got = jnp.zeros((b, nret), F32)
    gate = jnp.zeros((b, nret), F32)
    diag = _iota((b, b), 0) == _iota((b, b), 1)
    for j in range(k):
        pick = jnp.sum(jnp.where(diag, tk[j:j + 1, :], 0.0), axis=1, keepdims=True).astype(I32)
        gj = jnp.sum(jnp.where(diag, gates_t[j:j + 1, :], 0.0), axis=1, keepdims=True)
        same = glob == pick
        got = jnp.where(same, 1.0, got)
        gate = jnp.where(same, gj, gate)
    lower = jnp.where(_iota((b, b), 1) < _iota((b, b), 0), 1.0, 0.0).astype(BF)
    prior = _dot(lower, got.astype(BF))
    keep = (prior == lane_r) & (half - 2 * glob == core)
    gate = jnp.where(keep, gate, 0.0)
    g1 = gate.astype(BF)
    rest = gate - g1.astype(F32)
    g2 = rest.astype(BF)
    g3 = (rest - g2.astype(F32)).astype(BF)
    gmat[0:b] = g1
    gmat[b:2 * b] = g2
    gmat[2 * b:3 * b] = g3

    with jax.named_scope('barrier'):
        pl.semaphore_wait(barrier, ndev - 1)

    def across(src_ref, dst_ref, send, recv, dist, oc):
        return pltpu.make_async_remote_copy(
            src_ref=src_ref, dst_ref=dst_ref, send_sem=send, recv_sem=recv,
            device_id=peer(dist, oc)[0], device_id_type=MESH)

    def pcopy(dist):
        return across(tmine, tall.at[me], psend.at[dist], precv.at[dist], dist, 0)

    def qcopy(dist):
        src = peer(dist, 0)[1]
        return across(tmine if dist == 0 else tall.at[src], tall.at[src], qsend.at[dist], qrecv.at[dist], 0, 1)

    def ucopy(dist):
        return across(u, ug.at[me], usend.at[dist], urecv.at[dist], dist, 0)

    def vcopy(dist):
        src = peer(dist, 0)[1]
        return across(u if dist == 0 else ug.at[src], ug.at[src], vsend.at[dist], vrecv.at[dist], 0, 1)

    order = [7, 6, 5, 3, 4, 2, 1]
    arrive = [4, 2, 1, 6, 5, 3, 7]
    for dist in order:
        pcopy(dist).start()
    qcopy(0).start()
    for dist in order:
        ucopy(dist).start()
    vcopy(0).start()
    with jax.named_scope('choices'):
        for dist in arrive:
            pcopy(dist).wait_recv()
            qcopy(dist).start()
        for dist in range(nchip):
            qcopy(dist).wait_recv()

    with jax.named_scope('slots'):
        nh = lanes // b
        tok_e = jnp.concatenate(
            [functools.reduce(jnp.add, [tall[i * nh + n] for n in range(nh)]) for i in range(ndev // nh)], axis=1)
        row, colm = _iota((nslot, ntok), 0), _iota((nslot, ntok), 1)
        rsrc, rexp = lax.div(row, cap), lax.div(row, erow)
        want = (me * edev + rexp).astype(F32)
        hit = jnp.zeros((nslot, ntok), F32)
        for j in range(k):
            hit = jnp.where(want == tok_e[j:j + 1, :], 1.0, hit)
        ra, ca = _iota((ntok, ntok), 0), _iota((ntok, ntok), 1)
        earlier = jnp.where((lax.div(ra, b) == lax.div(ca, b)) & (ra < ca), 1.0, 0.0).astype(BF)
        before = _dot(hit.astype(BF), earlier)
        keep = (before == (row - rsrc * cap).astype(F32)) & (lax.div(colm, b) == rsrc - rexp * ndev)
        perm[...] = jnp.where(keep, hit, 0.0).astype(BF)

    with jax.named_scope('rows'):
        for dist in arrive:
            ucopy(dist).wait_recv()
            vcopy(dist).start()
    with jax.named_scope('rows_core'):
        for dist in range(nchip):
            vcopy(dist).wait_recv()

    nx = 4
    cx = d // nx
    with jax.named_scope('gather'):
      for n in range(nx):
        sl = slice(n * cx, (n + 1) * cx)
        xin[:, :, sl] = _dot(perm[...], ug[:, :, sl].reshape(ntok, cx)).astype(BF).reshape(edev, erow, cx)

    def rcopy(e, dist):
        chip = chips[dist]
        return pltpu.make_async_remote_copy(
            src_ref=oscr.at[e, chip], dst_ref=ret.at[me * edev + e],
            send_sem=rsend.at[e, dist], recv_sem=rrecv.at[e, dist],
            device_id=peer(dist, 0)[0], device_id_type=MESH)

    def tcopy(e, dist):
        src = peer(dist, 0)[1]
        at = src * edev + e
        return pltpu.make_async_remote_copy(
            src_ref=oscr.at[e, chip_me] if dist == 0 else ret.at[at], dst_ref=ret.at[at],
            send_sem=tsend.at[e, dist], recv_sem=trecv.at[e, dist],
            device_id=peer(0, 1)[0], device_id_type=MESH)

    def ffn(uv, i1, i3, i2, store):
        nz = 2
        cz = ff // nz
        zs = []
        for n in range(nz):
            sl = slice(n * cz, (n + 1) * cz)
            g = _dot(uv, wab[i1, :, sl])
            v = _dot(uv, wab[i3, :, sl])
            zs.append((g / (1.0 + jnp.exp(-g)) * v).astype(BF))
        z = jnp.concatenate(zs, axis=1)
        ny = 4
        cy = d // ny
        return z, ny, cy

    def forward(e):
        with jax.named_scope(f'forward#e={e}'):
            for dist in arrive:
                rcopy(e, dist).wait_recv()
                tcopy(e, dist).start()

    for e in range(edev):
        with jax.named_scope(f'weights#e={e}'):
            acopy(e, 0).wait()
            acopy(e, 1).wait()
        with jax.named_scope(f'up#e={e}'):
            z, ny, cy = ffn(xin[e], 2 * e, 2 * e + 1, e, None)
            ccopy(e).wait()
        with jax.named_scope(f'down#e={e}'):
            for n in range(ny):
                sl = slice(n * cy, (n + 1) * cy)
                oscr[e, :, :, sl] = _dot(z, wcb[e, :, sl]).astype(BF).reshape(nchip, 2 * cap, cy)
        if e == 0:
            for c in shared_copies():
                c.start()
        for dist in order:
            rcopy(e, dist).start()
        tcopy(e, 0).start()
        ret[me * edev + e] = oscr[e, chip_me]
        if e > 0:
            forward(e - 1)

    with jax.named_scope('shared'):
        sa, sb, sc = shared_copies()
        sa.wait()
        sb.wait()
        z, ny, cy = ffn(u[...], 0, 1, 0, None)
        sc.wait()
        shared = [_dot(z, wcb[0, :, n * cy:(n + 1) * cy]).astype(BF) for n in range(ny)]

    forward(edev - 1)
    with jax.named_scope('back_core'):
        for e in range(edev):
            for dist in range(nchip):
                tcopy(e, dist).wait_recv()
    with jax.named_scope('combine'):
        for n in range(ny):
            sl = slice(n * cy, (n + 1) * cy)
            r = _dot(gmat[...], ret[:, :, sl].reshape(nret, cy))
            routed = r[0:b] + r[b:2 * b] + r[2 * b:3 * b]
            y[:, sl] = (h[:, sl].astype(F32) + shared[n].astype(F32) + routed).astype(BF)

    for dist in range(1, nchip):
        pcopy(dist).wait_send()
        ucopy(dist).wait_send()
    for dist in range(nchip):
        qcopy(dist).wait_send()
        vcopy(dist).wait_send()
    for e in range(edev):
        for dist in range(1, nchip):
            rcopy(e, dist).wait_send()
        for dist in range(nchip):
            tcopy(e, dist).wait_send()


def _moe(h, u, topk, gates, ws1, ws3, ws2, w1, w3, w2, ndev, cap):
    b, d = h.shape
    edev, _, ff = w1.shape
    nchip = ndev // 2
    slots = edev * cap
    vm = pl.BlockSpec(memory_space=pltpu.VMEM)
    hbm = pl.BlockSpec(memory_space=pl.ANY)
    dma = pltpu.SemaphoreType.DMA
    return pl.pallas_call(
        functools.partial(_moe_kernel, cap),
        out_shape=jax.ShapeDtypeStruct((b, d), BF),
        in_specs=[vm] * 4 + [hbm] * 6,
        out_specs=vm,
        scratch_shapes=[
            pltpu.VMEM((2 * edev, d, ff), BF),
            pltpu.VMEM((edev, ff, d), BF),
            pltpu.VMEM((topk.shape[1], 128), F32),
            pltpu.VMEM((ndev, topk.shape[1], 128), F32),
            pltpu.VMEM((ndev * slots, ndev * b), BF),
            pltpu.VMEM((ndev, b, d), BF),
            pltpu.VMEM((edev, ndev * cap, d), BF),
            pltpu.VMEM((edev, nchip, 2 * cap, d), BF),
            pltpu.VMEM((ndev * edev, 2 * cap, d), BF),
            pltpu.VMEM((3 * b, ndev * edev * 2 * cap), BF),
            dma((edev + 1, 2)), dma((edev + 1,)),
            dma((nchip,)), dma((nchip,)), dma((nchip,)), dma((nchip,)),
            dma((nchip,)), dma((nchip,)), dma((nchip,)), dma((nchip,)),
            dma((edev, nchip)), dma((edev, nchip)), dma((edev, nchip)), dma((edev, nchip)),
        ],
        compiler_params=pltpu.CompilerParams(
            collective_id=0, has_side_effects=True, vmem_limit_bytes=VMEM_LIMIT),
        cost_estimate=pl.CostEstimate(
            flops=6 * (edev * ndev * cap + b) * d * ff, bytes_accessed=6 * (edev + 1) * d * ff, transcendentals=0),
        name='experts',
    )(h, u, topk.T, gates.T, ws1, ws3, ws2, w1, w3, w2)


def solution(mesh):
    ndev = mesh.shape['ey'] * mesh.shape['ex']
    rows = P(('ey', 'ex'))
    rep = P()

    def local(x, kv_k, kv_v, lens, topk_idx, gates, ln1, ln2, wq, wo, ws1, ws3, ws2, w1, w3, w2):
        cap = 4
        h, u = _attention(x, kv_k, kv_v, lens, ln1, ln2, wq, wo)
        return _moe(h, u, topk_idx, gates, ws1, ws3, ws2, w1, w3, w2, ndev, cap)

    return jax.shard_map(
        local, mesh=mesh,
        in_specs=(rows, rows, rows, rows, rows, rows, rep, rep, rep, rep, rep, rep, rep, rows, rows, rows),
        out_specs=rows, check_vma=False)
```

```python
import functools

import jax
import jax.numpy as jnp
from jax import lax
from jax.experimental import pallas as pl
from jax.experimental.pallas import tpu as pltpu
from jax.sharding import PartitionSpec as P

EPS = 1e-6
BF = jnp.bfloat16
F32 = jnp.float32
I32 = jnp.int32
MESH = pl.DeviceIdType.MESH
VMEM_LIMIT = 60 * 1024 * 1024

SHORT = 32


def _iota(shape, dim):
    return lax.broadcasted_iota(I32, shape, dim)


def _dot(a, b):
    return jnp.dot(a, b, preferred_element_type=F32)


def _rms(v, w):
    v = v.astype(F32)
    r = lax.rsqrt(jnp.mean(v * v, axis=-1, keepdims=True) + EPS)
    w = w.astype(F32)
    n = w.shape[1]
    parts = [(v[:, i * n:(i + 1) * n] * r * w[i:i + 1, :]).astype(BF) for i in range(w.shape[0])]
    return jnp.concatenate(parts, axis=1)


def _attn_kernel(lens, x_in, ln1_in, ln2_in, kk, vv, wq, wo, h_out, u_out,
                 kbuf, vbuf, wqb, wob, x, ln1, ln2, q3, o3, posd, longs,
                 isem, wsem, osem, ssem, lsem):
    b, heads, dh = q3.shape
    rows = kbuf.shape[1]
    short = SHORT * heads
    d = x.shape[1]
    nw = wsem.shape[0]
    cw = d // nw
    scale = dh ** -0.5

    def wcopy(n):
        return pltpu.make_async_copy(wq.at[:, pl.ds(n * cw, cw)], wqb.at[:, pl.ds(n * cw, cw)], wsem.at[n])

    def scopy(i, t):
        src, dst = ((kk, kbuf), (vv, vbuf))[i]
        return pltpu.make_async_copy(src.at[t, pl.ds(0, short)], dst.at[t, pl.ds(0, short)], ssem)

    def lcopy(i, t):
        src, dst = ((kk, kbuf), (vv, vbuf))[i]
        rest = pl.ds(short, rows - short)
        return pltpu.make_async_copy(src.at[t, rest], dst.at[t, rest], lsem.at[t])

    small = [pltpu.make_async_copy(s, t, isem) for s, t in ((x_in, x), (ln1_in, ln1), (ln2_in, ln2))]
    out_w = pltpu.make_async_copy(wo, wob, osem)
    for c in small:
        c.start()
    for n in range(nw):
        wcopy(n).start()
    for t in range(b):
        scopy(0, t).start()
        scopy(1, t).start()

    def scan(t, n):
        @pl.when(lens[t] > SHORT)
        def _():
            longs[n] = t
            lcopy(0, t).start()
            lcopy(1, t).start()
        return n + (lens[t] > SHORT).astype(I32)

    nlong = lax.fori_loop(0, b, scan, jnp.int32(0))
    out_w.start()

    pr, pc = _iota(posd.shape, 0), _iota(posd.shape, 1)
    pos = lax.div(pc, heads)
    posd[...] = jnp.where(pc - pos * heads == lax.rem(pr, heads), pos, jnp.int32(1 << 20))
    upper = _iota((2 * heads, 1), 0) >= heads

    for c in small:
        c.wait()
    a = _rms(x[...], ln1[...])
    for n in range(nw):
        with jax.named_scope(f'wait_wq#n={n}'):
            wcopy(n).wait()
        q = _dot(a, wqb[:, n * cw:(n + 1) * cw]).astype(BF).astype(F32)
        for i in range(cw // dh):
            q3[:, n * (cw // dh) + i, :] = q[:, i * dh:(i + 1) * dh]

    def both(f, v):
        m = f(v[:heads], v[heads:])
        return jnp.concatenate([m, m], axis=0)

    def scores(t, m):
        hm = m // 2
        qt = q3[t].astype(BF)
        none = jnp.zeros_like(qt)
        qq = jnp.concatenate([jnp.concatenate([qt, none], axis=1), jnp.concatenate([none, qt], axis=1)], axis=0)
        kc = jnp.concatenate([kbuf[t, :hm], kbuf[t, hm:m]], axis=1)
        s = lax.dot_general(qq, kc, (((1,), (1,)), ((), ())), preferred_element_type=F32)
        bound = jnp.where(upper, lens[t] - hm // heads, lens[t])
        s = jnp.where(posd[:, :hm] < bound, s * scale, -jnp.inf)
        top = both(jnp.maximum, jnp.max(s, axis=-1, keepdims=True))
        e = jnp.exp(s - top)
        return (e / both(jnp.add, jnp.sum(e, axis=-1, keepdims=True))).astype(BF)

    def attend(ts, m):
        hm = m // 2
        ps = [scores(t, m) for t in ts]
        for t, p in zip(ts, ps):
            vc = jnp.concatenate([vbuf[t, :hm], vbuf[t, hm:m]], axis=1)
            r = _dot(p, vc)
            o3[t] = (r[:heads, :dh] + r[heads:, dh:]).astype(BF).astype(F32)

    with jax.named_scope('wait_short'):
        for t in range(b):
            scopy(0, t).wait()
            scopy(1, t).wait()
    group = 8
    with jax.named_scope('short'):
        for t0 in range(0, b, group):
            attend(list(range(t0, t0 + group)), short)

    def long_pair(j, carry):
        first = 2 * j
        second = jnp.minimum(first + 1, nlong - 1)
        t0, t1 = longs[first], longs[second]
        with jax.named_scope('wait_long'):
            lcopy(0, t0).wait()
            lcopy(1, t0).wait()

            @pl.when(second > first)
            def _():
                lcopy(0, t1).wait()
                lcopy(1, t1).wait()
        with jax.named_scope('long'):
            attend([t0, t1], rows)
        return carry

    lax.fori_loop(0, (nlong + 1) // 2, long_pair, 0)

    with jax.named_scope('wait_wo'):
        out_w.wait()
    with jax.named_scope('wo'):
        o = jnp.concatenate([o3[:, i, :].astype(BF) for i in range(heads)], axis=1)
        no = 2
        co = d // no
        for n in range(no):
            sl = slice(n * co, (n + 1) * co)
            h_out[:, sl] = (x[:, sl].astype(F32) + _dot(o, wob[:, sl])).astype(BF)
        u_out[...] = _rms(h_out[...], ln2[...])


def _attention(x, kk, vv, lens, ln1, ln2, wq, wo):
    b, d = x.shape
    _, l, heads, dh = kk.shape
    rows = l * heads
    vm = pl.BlockSpec(memory_space=pltpu.VMEM)
    hbm = pl.BlockSpec(memory_space=pl.ANY)
    nbytes = 2 * (2 * b * rows * dh + 2 * d * d)
    dma = pltpu.SemaphoreType.DMA
    return pl.pallas_call(
        _attn_kernel,
        out_shape=[jax.ShapeDtypeStruct((b, d), BF)] * 2,
        in_specs=[pl.BlockSpec(memory_space=pltpu.SMEM)] + [hbm] * 7,
        out_specs=[vm, vm],
        scratch_shapes=[
            pltpu.VMEM((b, rows, dh), BF),
            pltpu.VMEM((b, rows, dh), BF),
            pltpu.VMEM((d, d), BF),
            pltpu.VMEM((d, d), BF),
            pltpu.VMEM((b, d), BF),
            pltpu.VMEM((d // 128, 128), BF),
            pltpu.VMEM((d // 128, 128), BF),
            pltpu.VMEM((b, heads, dh), F32),
            pltpu.VMEM((b, heads, dh), F32),
            pltpu.VMEM((2 * heads, rows // 2), I32),
            pltpu.SMEM((b,), I32),
            dma, dma((4,)), dma, dma, dma((b,)),
        ],
        compiler_params=pltpu.CompilerParams(vmem_limit_bytes=VMEM_LIMIT),
        cost_estimate=pl.CostEstimate(flops=4 * b * d * d, bytes_accessed=nbytes, transcendentals=0),
        name='attention',
    )(lens, x, ln1.reshape(d // 128, 128), ln2.reshape(d // 128, 128),
      kk.reshape(b, rows, dh), vv.reshape(b, rows, dh), wq, wo)


def _moe_kernel(cap, h_in, u_in, topk_in, gates_in, ws1, ws3, ws2, w1, w3, w2, y,
                wab, wcb, h, u, topk_t, gates_t, tmine, tall, perm, ug, xin, oscr, ret, gmat, acc,
                isem, usem, asem, csem, psend, precv, qsend, qrecv, usend, urecv, vsend, vrecv,
                rsend, rrecv, tsend, trecv):
    b, d = h.shape
    k = topk_t.shape[0]
    edev = w1.shape[0]
    ff = w1.shape[2]
    ndev = ug.shape[0]
    nchip = ndev // 2
    ntok = ndev * b
    slots = edev * cap
    nslot = ndev * slots
    erow = ndev * cap
    ey, ex = lax.axis_index('ey'), lax.axis_index('ex')
    nex = nchip
    iy = lax.div(ex, 4)
    ix = lax.div(ex, 2) - 2 * iy
    core = lax.rem(ex, 2)
    me = ey * nex + ex
    chip_me = lax.div(me, 2)

    flip = lambda i, by: 1 - i if by else i
    peers = {}
    for dist in range(nchip):
        pz, py, px = flip(ey, dist // 4), flip(iy, dist // 2 % 2), flip(ix, dist % 2)
        for oc in range(2):
            pex = py * 4 + px * 2 + flip(core, oc)
            peers[dist, oc] = ((pz, pex), pz * nex + pex)
    chips = [lax.div(peers[dist, 0][1], 2) for dist in range(nchip)]

    def peer(dist, other_core):
        return peers[dist, other_core]

    def acopy(e, i):
        return pltpu.make_async_copy((w1, w3)[i].at[e], wab.at[2 * e + i], asem.at[e])

    def ccopy(e):
        return pltpu.make_async_copy(w2.at[e], wcb.at[e], csem.at[e])

    def shared_copies():
        return [pltpu.make_async_copy(ws1, wab.at[0], asem.at[edev]),
                pltpu.make_async_copy(ws3, wab.at[1], asem.at[edev]),
                pltpu.make_async_copy(ws2, wcb.at[0], csem.at[edev])]

    def drained(ref, sem):
        pltpu.make_async_copy(ref, ref, sem).wait()

    barrier = pltpu.get_barrier_semaphore()
    for dist in range(nchip):
        for oc in range(2):
            if dist or oc:
                pl.semaphore_signal(barrier, inc=1, device_id=peer(dist, oc)[0], device_id_type=MESH)

    small = [pltpu.make_async_copy(s, t, isem.at[i])
             for i, (s, t) in enumerate(((topk_in, topk_t), (gates_in, gates_t), (h_in, h)))]
    rows_in = pltpu.make_async_copy(u_in, u, usem)
    rows_in.start()
    for c in small:
        c.start()
    for e in range(edev):
        acopy(e, 0).start()
        acopy(e, 1).start()
        ccopy(e).start()
    for c in small:
        c.wait()

    lanes = tmine.shape[1]
    tk = topk_t[...].astype(F32)
    rep_r, rep_c = _iota((b, lanes), 0), _iota((b, lanes), 1)
    block = me - lax.div(me, lanes // b) * (lanes // b)
    spread = jnp.where(rep_c - block * b == rep_r, 1.0, 0.0).astype(BF)
    tmine[...] = _dot(tk.astype(BF), spread)
    tall[me] = tmine[...]

    nret = ndev * 2 * cap
    lane = _iota((b, edev * nret), 1)
    tile = lax.div(lane, 2 * cap)
    expert = lax.div(lane, nret)
    glob = (tile - expert * ndev) * edev + expert
    half = lax.div(lane, cap)
    lane_r = (lane - half * cap).astype(F32)
    got = jnp.zeros((b, edev * nret), F32)
    gate = jnp.zeros((b, edev * nret), F32)
    diag = _iota((b, b), 0) == _iota((b, b), 1)
    for j in range(k):
        pick = jnp.sum(jnp.where(diag, tk[j:j + 1, :], 0.0), axis=1, keepdims=True).astype(I32)
        gj = jnp.sum(jnp.where(diag, gates_t[j:j + 1, :], 0.0), axis=1, keepdims=True)
        same = glob == pick
        got = jnp.where(same, 1.0, got)
        gate = jnp.where(same, gj, gate)
    lower = jnp.where(_iota((b, b), 1) < _iota((b, b), 0), 1.0, 0.0).astype(BF)
    prior = _dot(lower, got.astype(BF))
    keep = (prior == lane_r) & (half - 2 * tile == core)
    gate = jnp.where(keep, gate, 0.0)
    g1 = gate.astype(BF)
    rest = gate - g1.astype(F32)
    g2 = rest.astype(BF)
    g3 = (rest - g2.astype(F32)).astype(BF)
    gmat[0:b] = g1
    gmat[b:2 * b] = g2
    gmat[2 * b:3 * b] = g3

    with jax.named_scope('barrier'):
        pl.semaphore_wait(barrier, ndev - 1)

    def across(src_ref, dst_ref, send, recv, dist, oc):
        return pltpu.make_async_remote_copy(
            src_ref=src_ref, dst_ref=dst_ref, send_sem=send, recv_sem=recv,
            device_id=peer(dist, oc)[0], device_id_type=MESH)

    def pcopy(dist):
        return across(tmine, tall.at[me], psend, precv.at[dist], dist, 0)

    def qcopy(dist):
        src = peer(dist, 0)[1]
        return across(tmine if dist == 0 else tall.at[src], tall.at[src], qsend, qrecv, 0, 1)

    via = {3: (1, 2), 6: (2, 4), 5: (4, 1)}

    def ucopy(dist):
        if dist in via:
            first, link = via[dist]
            src = peer(first, 0)[1]
            return across(ug.at[src], ug.at[src], usend, urecv.at[dist], link, 0)
        return across(u, ug.at[me], usend, urecv.at[dist], dist, 0)

    def vcopy(dist):
        src = peer(dist, 0)[1]
        return across(u if dist == 0 else ug.at[src], ug.at[src], vsend, vrecv, 0, 1)

    order = [7, 6, 5, 3, 4, 2, 1]
    arrive = [4, 2, 1, 6, 5, 3, 7]
    for dist in order:
        pcopy(dist).start()
    qcopy(0).start()
    rows_in.wait()
    for dist in [1, 2, 4, 7]:
        ucopy(dist).start()
    vcopy(0).start()
    ug[me] = u[...]
    with jax.named_scope('rows_near'):
        for dist in [3, 6, 5]:
            first = via[dist][0]
            ucopy(first).wait_recv()
            ucopy(dist).start()
            vcopy(first).start()
    with jax.named_scope('choices'):
        for dist in arrive:
            pcopy(dist).wait_recv()
            qcopy(dist).start()
        drained(tall.at[pl.ds(0, nchip)], qrecv)

    with jax.named_scope('slots'):
        nh = lanes // b
        tok_e = jnp.concatenate(
            [functools.reduce(jnp.add, [tall[i * nh + n] for n in range(nh)]) for i in range(ndev // nh)], axis=1)
        row, colm = _iota((nslot, ntok), 0), _iota((nslot, ntok), 1)
        rsrc, rexp = lax.div(row, cap), lax.div(row, erow)
        want = (me * edev + rexp).astype(F32)
        hit = jnp.zeros((nslot, ntok), F32)
        for j in range(k):
            hit = jnp.where(want == tok_e[j:j + 1, :], 1.0, hit)
        ra, ca = _iota((ntok, ntok), 0), _iota((ntok, ntok), 1)
        earlier = jnp.where((lax.div(ra, b) == lax.div(ca, b)) & (ra < ca), 1.0, 0.0).astype(BF)
        before = _dot(hit.astype(BF), earlier)
        keep = (before == (row - rsrc * cap).astype(F32)) & (lax.div(colm, b) == rsrc - rexp * ndev)
        perm[...] = jnp.where(keep, hit, 0.0).astype(BF)

    with jax.named_scope('rows'):
        for dist in [7, 3, 6, 5]:
            ucopy(dist).wait_recv()
            vcopy(dist).start()
    with jax.named_scope('rows_core'):
        drained(ug.at[pl.ds(0, nchip)], vrecv)

    nx = 4
    cx = d // nx
    with jax.named_scope('gather'):
      for n in range(nx):
        sl = slice(n * cx, (n + 1) * cx)
        xin[:, :, sl] = _dot(perm[...], ug[:, :, sl].reshape(ntok, cx)).astype(BF).reshape(edev, erow, cx)

    def rcopy(e, dist):
        return across(oscr.at[e, chips[dist]], ret.at[e, me], rsend, rrecv.at[e, dist], dist, 0)

    def tcopy(e, dist):
        src = peer(dist, 0)[1]
        return across(oscr.at[e, chip_me] if dist == 0 else ret.at[e, src], ret.at[e, src],
                      tsend, trecv.at[e], 0, 1)

    def ffn(uv, i1, i3):
        nz = 2
        cz = ff // nz
        zs = []
        for n in range(nz):
            sl = slice(n * cz, (n + 1) * cz)
            g = _dot(uv, wab[i1, :, sl])
            v = _dot(uv, wab[i3, :, sl])
            zs.append((g / (1.0 + jnp.exp(-g)) * v).astype(BF))
        return jnp.concatenate(zs, axis=1)

    def forward(e):
        with jax.named_scope(f'forward#e={e}'):
            for dist in arrive:
                rcopy(e, dist).wait_recv()
                tcopy(e, dist).start()

    ny = 4
    cy = d // ny
    for e in range(edev):
        with jax.named_scope(f'weights#e={e}'):
            drained(wab.at[pl.ds(2 * e, 2)], asem.at[e])
        with jax.named_scope(f'up#e={e}'):
            z = ffn(xin[e], 2 * e, 2 * e + 1)
            ccopy(e).wait()
        with jax.named_scope(f'down#e={e}'):
            for n in range(ny):
                sl = slice(n * cy, (n + 1) * cy)
                oscr[e, :, :, sl] = _dot(z, wcb[e, :, sl]).astype(BF).reshape(nchip, 2 * cap, cy)
        if e == 0:
            for c in shared_copies():
                c.start()
        for dist in order:
            rcopy(e, dist).start()
        tcopy(e, 0).start()
        ret[e, me] = oscr[e, chip_me]

    def add(e):
        with jax.named_scope(f'add#e={e}'):
            drained(ret.at[e, pl.ds(0, nchip)], trecv.at[e])
            for n in range(ny):
                sl = slice(n * cy, (n + 1) * cy)
                r = _dot(gmat[:, e * nret:(e + 1) * nret], ret[e, :, :, sl].reshape(nret, cy))
                r = acc[:, sl] + (r[0:b] + r[b:2 * b] + r[2 * b:3 * b])
                if e < edev - 1:
                    acc[:, sl] = r
                else:
                    y[:, sl] = r.astype(BF)

    forward(0)
    with jax.named_scope('shared'):
        drained(wab.at[pl.ds(0, 2)], asem.at[edev])
        z = ffn(u[...], 0, 1)
        shared_copies()[2].wait()
        for n in range(ny):
            sl = slice(n * cy, (n + 1) * cy)
            acc[:, sl] = h[:, sl].astype(F32) + _dot(z, wcb[0, :, sl]).astype(BF).astype(F32)
    for e in range(1, edev):
        forward(e)
        add(e - 1)
    add(edev - 1)

    with jax.named_scope('sent'):
        drained(tall.at[pl.ds(0, nchip - 1)], psend)
        drained(tall.at[pl.ds(0, nchip)], qsend)
        drained(ug.at[pl.ds(0, nchip - 1)], usend)
        drained(ug.at[pl.ds(0, nchip)], vsend)
        drained(oscr.at[:, pl.ds(0, nchip - 1)], rsend)
        drained(oscr, tsend)


def _moe(h, u, topk, gates, ws1, ws3, ws2, w1, w3, w2, ndev, cap):
    b, d = h.shape
    k = topk.shape[1]
    edev, _, ff = w1.shape
    nchip = ndev // 2
    slots = edev * cap
    vm = pl.BlockSpec(memory_space=pltpu.VMEM)
    hbm = pl.BlockSpec(memory_space=pl.ANY)
    dma = pltpu.SemaphoreType.DMA
    return pl.pallas_call(
        functools.partial(_moe_kernel, cap),
        out_shape=jax.ShapeDtypeStruct((b, d), BF),
        in_specs=[hbm] * 10,
        out_specs=vm,
        scratch_shapes=[
            pltpu.VMEM((2 * edev, d, ff), BF),
            pltpu.VMEM((edev, ff, d), BF),
            pltpu.VMEM((b, d), BF),
            pltpu.VMEM((b, d), BF),
            pltpu.VMEM((k, b), I32),
            pltpu.VMEM((k, b), F32),
            pltpu.VMEM((k, 128), F32),
            pltpu.VMEM((ndev, k, 128), F32),
            pltpu.VMEM((ndev * slots, ndev * b), BF),
            pltpu.VMEM((ndev, b, d), BF),
            pltpu.VMEM((edev, ndev * cap, d), BF),
            pltpu.VMEM((edev, nchip, 2 * cap, d), BF),
            pltpu.VMEM((edev, ndev, 2 * cap, d), BF),
            pltpu.VMEM((3 * b, edev * ndev * 2 * cap), BF),
            pltpu.VMEM((b, d), F32),
            dma((3,)), dma, dma((edev + 1,)), dma((edev + 1,)),
            dma, dma((nchip,)), dma, dma,
            dma, dma((nchip,)), dma, dma,
            dma, dma((edev, nchip)), dma, dma((edev,)),
        ],
        compiler_params=pltpu.CompilerParams(
            collective_id=0, has_side_effects=True, vmem_limit_bytes=VMEM_LIMIT),
        cost_estimate=pl.CostEstimate(
            flops=6 * (edev * ndev * cap + b) * d * ff, bytes_accessed=6 * (edev + 1) * d * ff, transcendentals=0),
        name='experts',
    )(h, u, topk.T, gates.T, ws1, ws3, ws2, w1, w3, w2)


def solution(mesh):
    ndev = mesh.shape['ey'] * mesh.shape['ex']
    rows = P(('ey', 'ex'))
    rep = P()

    def local(x, kv_k, kv_v, lens, topk_idx, gates, ln1, ln2, wq, wo, ws1, ws3, ws2, w1, w3, w2):
        cap = 4
        h, u = _attention(x, kv_k, kv_v, lens, ln1, ln2, wq, wo)
        return _moe(h, u, topk_idx, gates, ws1, ws3, ws2, w1, w3, w2, ndev, cap)

    return jax.shard_map(
        local, mesh=mesh,
        in_specs=(rows, rows, rows, rows, rows, rows, rep, rep, rep, rep, rep, rep, rep, rows, rows, rows),
        out_specs=rows, check_vma=False)
```
